128 devices in a mesh: groups: 4 (over y, x), tp: 16 (over z), blk: 2 (over core).
Axes of the slice: x: 2, y: 2, z: 16, core: 2. Of those that a mesh axis runs over, the one named last changes fastest.
The devices are a block of a 8x8x16 slice.
Arguments:
- tokens: bfloat16 [16384, 7168], P(('groups', 'tp')), parts along dimension 0, may hold values from -6 to 6
- gate_weight: bfloat16 [7168, 2048], P('tp', 'blk'), may hold values from -0.0625 to 0.0625
- up_weight: bfloat16 [7168, 2048], P('tp', 'blk'), may hold values from -0.0625 to 0.0625
- down_weight: bfloat16 [2048, 7168], P('blk', 'tp'), may hold values from -0.125 to 0.125
Outputs:
- mixed: bfloat16 [16384, 7168], P(('groups', 'blk'), 'tp'), parts along dimension 0
The draws below stay inside these ranges and needn't reach their ends.
There are 4 independent parts, one for each index of `groups`. The reference program is written for one: setup_inputs(seed, part) draws one part's arguments, and reference() takes and returns one part's arrays. A program takes and returns all parts, laid end to end along the dimension named above; an argument that names none is the same for every part. Nothing has to cross between parts.
All inputs are finite; a program needn't handle non-finite values.
Results may differ from the reference program's by a relative error of at most 0.005.
Values may be sent and summed in bfloat16 or wider, within the bound.
A program may use at most 128 MiB of HBM per device.

```python
import jax
import jax.numpy as jnp

D = 7168
FF = 2048
TOKENS = 4096


def shard_levels(key, extent, shards, least, top_value):
    gain, own = 1.0, jax.random.fold_in(key, 6)
    for position, blocks in shards:
        heights = jnp.exp(jax.random.uniform(jax.random.fold_in(own, position), (blocks,), jnp.float32, least / len(shards), top_value / len(shards)))
        gain = gain * jnp.repeat(heights, extent[position] // blocks).reshape([-1 if axis == position else 1 for axis in range(len(extent))])
    return gain


def bell_draw(stream_key, shape, spread, bound, cuts=(), dtype=jnp.bfloat16):
    factor_of = shard_levels(stream_key, shape, cuts, -0.22, 0.18) if cuts else 1.0
    array = jax.random.normal(stream_key, shape, jnp.float32) * spread * factor_of
    return jnp.minimum(jnp.maximum(array, -bound), bound).astype(dtype)


def setup_inputs(seed: int = 0, part: int = 0) -> dict:
    key_list = jax.random.split(jax.random.key(seed), 5)
    own_keys = jax.random.split(jax.random.fold_in(key_list[4], part), 5)
    tokens = bell_draw(own_keys[0], (TOKENS, D), 1.0, 6.0, ((0, 16),))
    gate_weight = bell_draw(key_list[1], (D, FF), D ** -0.5, 0.0625, ((0, 16), (1, 2)))
    up_weight = bell_draw(key_list[2], (D, FF), D ** -0.5, 0.0625, ((0, 16), (1, 2)))
    down_weight = bell_draw(key_list[3], (FF, D), FF ** -0.5, 0.125, ((0, 2), (1, 16)))
    return dict(tokens=tokens, gate_weight=gate_weight, up_weight=up_weight, down_weight=down_weight)


def reference(tokens, gate_weight, up_weight, down_weight):
    gate = jnp.dot(tokens, gate_weight, preferred_element_type=jnp.float32)
    up = jnp.dot(tokens, up_weight, preferred_element_type=jnp.float32)
    hidden = (jax.nn.silu(gate) * up).astype(jnp.bfloat16)
    return jnp.dot(hidden, down_weight, preferred_element_type=jnp.float32).astype(jnp.bfloat16)
```

```python
import math

import jax
import jax.numpy as jnp
from jax import lax
from jax.sharding import PartitionSpec as P


def quads_of(groups):
    side = math.isqrt(groups)
    return [
        [y * side + x, y * side + x + 1, (y + 1) * side + x, (y + 1) * side + x + 1]
        for y in range(0, side, 2)
        for x in range(0, side, 2)
    ]


def local(groups, tokens, gate_weight, up_weight, down_weight):
    quads = quads_of(groups)
    side = math.isqrt(groups)
    g = lax.axis_index("groups")
    place = (g // side) % 2 * 2 + g % 2
    width = gate_weight.shape[1] // 4
    own = jnp.concatenate(
        [
            lax.dynamic_slice_in_dim(gate_weight, place * width, width, 1),
            lax.dynamic_slice_in_dim(up_weight, place * width, width, 1),
        ],
        axis=1,
    )
    weights = lax.all_gather(own, "tp", axis=0, tiled=True)
    rows = lax.all_gather(tokens, "groups", axis=0, tiled=True, axis_index_groups=quads)
    both = jnp.dot(rows, weights, preferred_element_type=jnp.float32)
    hidden = (jax.nn.silu(both[:, :width]) * both[:, width:]).astype(jnp.bfloat16)
    hidden = lax.all_to_all(
        hidden, "groups", split_axis=0, concat_axis=1, tiled=True, axis_index_groups=quads
    )
    gathered = lax.all_gather(hidden, "tp", axis=0, tiled=True)
    own_units = lax.all_to_all(gathered, "blk", split_axis=0, concat_axis=1, tiled=True)
    down_full = lax.all_gather(down_weight, "blk", axis=0, tiled=True)
    result = jnp.dot(own_units, down_full, preferred_element_type=jnp.float32)
    return result.astype(jnp.bfloat16)


def solution(mesh):
    groups = mesh.shape["groups"]
    return jax.shard_map(
        lambda *a: local(groups, *a),
        mesh=mesh,
        in_specs=(P(("groups", "tp"), None), P("tp", "blk"), P("tp", "blk"), P("blk", "tp")),
        out_specs=P(("groups", "blk"), "tp"),
        check_vma=False,
    )
```

```python
import functools
import math

import jax
import jax.numpy as jnp
from jax import lax
from jax.experimental import pallas as pl
from jax.experimental.pallas import tpu as pltpu
from jax.sharding import PartitionSpec as P

MESH = pl.DeviceIdType.MESH
UNITS = 128


def kernel(side, n, tokens, gate, up, down, out, x, w, hid, peer, made, down_v, result,
           load_sem, w_send, w_recv, x_send, x_recv, xp_send, xp_recv, q_send, q_recv,
           h_send, h_recv, p_send, p_recv, d_send, d_recv, out_sem):
    last = n // 2
    rows, width = tokens.shape
    depth = gate.shape[0]
    half = down.shape[0] // 2
    piece = rows // 4

    g = lax.axis_index("groups")
    z = lax.axis_index("tp")
    c = lax.axis_index("blk")
    px = lax.rem(lax.rem(g, side), 2)
    py = lax.rem(lax.div(g, side), 2)
    place = 2 * py + px
    gx = g + 1 - 2 * px
    gy = g + side * (1 - 2 * py)
    gd = gx + side * (1 - 2 * py)
    mates = (None, gx, gy, gd)
    mate_place = (place, 2 * py + 1 - px, 2 * (1 - py) + px, 2 * (1 - py) + 1 - px)
    ahead, behind = lax.rem(z + 1, n), lax.rem(z + n - 1, n)
    to = (ahead, behind)

    def source(s, d):
        return lax.rem(z + n - s, n) if d == 0 else lax.rem(z + s, n)

    barrier = pltpu.get_barrier_semaphore()
    for target in ({"tp": ahead}, {"tp": behind}, {"groups": gx}, {"groups": gy}, {"groups": gd}, {"blk": 1 - c}):
        pl.semaphore_signal(barrier, inc=1, device_id=target, device_id_type=MESH)
    pl.semaphore_wait(barrier, 6)

    def remote(src, dst, send, recv, target):
        return pltpu.make_async_remote_copy(
            src_ref=src, dst_ref=dst, send_sem=send, recv_sem=recv, device_id=target, device_id_type=MESH
        )

    def w_own(f, u):
        first = pl.multiple_of(f * half + place * UNITS, UNITS)
        return (gate, up)[u].at[:, pl.ds(first, UNITS)]

    def w_at(f, u, block):
        return w.at[f, pl.ds(pl.multiple_of(block * depth, 64), depth), pl.ds(u * UNITS, UNITS)]

    def w_copy(f, s, u, d, block, src=None):
        there = w_at(f, u, block)
        return remote(there if src is None else src, there,
                      w_send.at[f, d, s - 1, u], w_recv.at[f, d, s - 1, u], {"tp": to[d]})

    def w_first(f, u):
        for d in range(2):
            w_copy(f, 1, u, d, z, w_own(f, u)).start()

    def w_step(f, s, stage):
        for u in range(2):
            for d in range(2):
                if stage == "end" and u != d:
                    continue
                block = source(s, d)
                w_copy(f, s, u, d, block).wait_recv()
                if stage == "on" or (stage == "near" and u == d):
                    w_copy(f, s + 1, u, d, block).start()

    def w_steps(f, low, high):
        def body(s, carry):
            w_step(f, s, "on")
            return carry
        lax.fori_loop(low, high, body, 0)

    def x_rows(core, part):
        return pl.ds(pl.multiple_of(core * (2 * piece) + part * piece, piece), piece)

    pieces = ((1, 0, gx), (1, 1, gx), (2, 1, gy), (2, 0, gy), (3, 1, gx), (3, 0, gy))

    def x_copy(i, src):
        slot, part, target = pieces[i]
        return remote(src, x.at[slot, x_rows(c, part)], x_send.at[i], x_recv.at[i], {"groups": target})

    def x_mine(i):
        slot, part, _ = pieces[i]
        return x.at[slot, x_rows(c, part)]

    def x_own(i):
        return tokens.at[x_rows(c, pieces[i][1])]

    def x_pass(i):
        return remote(x_mine(i), x_mine(i), xp_send.at[i], xp_recv.at[i], {"blk": 1 - c})

    def x_pass_in(i):
        slot, part, _ = pieces[i]
        there = x.at[slot, x_rows(1 - c, part)]
        return remote(there, there, xp_send.at[i], xp_recv.at[i], {"blk": 1 - c})

    def lanes(p):
        return pl.ds(pl.multiple_of(p * UNITS, UNITS), UNITS)

    def compute(f, r):
        both = jnp.dot(x[r], w[f], preferred_element_type=jnp.float32)
        a, b = both[:, :UNITS], both[:, UNITS:]
        h = (a / (1.0 + jnp.exp(-a)) * b).astype(jnp.bfloat16)
        if r == 0:
            hid[z, f, :, lanes(place)] = h
        else:
            made[f, r - 1] = h

    def q_copy(f, r):
        return remote(made.at[f, r - 1], hid.at[z, f, :, lanes(place)],
                      q_send.at[f, r - 1], q_recv.at[f, r - 1], {"groups": mates[r]})

    def q_in(f, r):
        there = hid.at[z, f, :, lanes(mate_place[r])]
        return remote(there, there, q_send.at[f, r - 1], q_recv.at[f, r - 1], {"groups": mates[r]})

    def h_copy(f, s, u, d, block):
        there = hid.at[block, f, :, lanes(mate_place[u])]
        return remote(there, there, h_send.at[f, d, s - 1, u], h_recv.at[f, d, s - 1, u], {"tp": to[d]})

    def h_first(f, u):
        for d in range(2):
            h_copy(f, 1, u, d, z).start()

    def h_takes(u, d):
        return u // 2 == d

    def h_step(f, s, stage):
        for u in range(4):
            for d in range(2):
                if stage == "end" and not h_takes(u, d):
                    continue
                block = source(s, d)
                h_copy(f, s, u, d, block).wait_recv()
                if stage == "on" or (stage == "near" and h_takes(u, d)):
                    h_copy(f, s + 1, u, d, block).start()

    def p_copy(f, block):
        at = lax.rem(block, last)
        return remote(hid.at[block, f], peer.at[at, f], p_send.at[at, f], p_recv.at[at, f], {"blk": 1 - c})

    def is_mine(block):
        return lax.div(block, last) == c

    def hand_over(f, block):
        @pl.when(jnp.logical_not(is_mine(block)))
        def _():
            p_copy(f, block).start()

    def out_copy(block):
        at = lax.rem(block, last)
        there = out.at[pl.ds(pl.multiple_of(at * rows, rows), rows)]
        return pltpu.make_async_copy(result.at[at], there, out_sem.at[at])

    def finish(block):
        @pl.when(is_mine(block))
        def _():
            at = lax.rem(block, last)
            p_copy(0, block).wait_recv()
            p_copy(1, block).wait_recv()
            total = jnp.zeros((rows, down.shape[1]), jnp.float32)
            for f in range(2):
                total += jnp.dot(hid[block, f], down_v[0, f * half:(f + 1) * half], preferred_element_type=jnp.float32)
                total += jnp.dot(peer[at, f], down_v[1, f * half:(f + 1) * half], preferred_element_type=jnp.float32)
            result[at] = total.astype(jnp.bfloat16)
            out_copy(block).start()

    w_first(0, 0)
    for i in (0, 2):
        x_copy(i, x_own(i)).start()
    w_first(0, 1)
    for i in (1, 3):
        x_copy(i, x_own(i)).start()
    w_first(1, 0)
    loads = [pltpu.make_async_copy(tokens, x.at[0], load_sem.at[0]),
             pltpu.make_async_copy(down, down_v.at[0], load_sem.at[1])]
    for f in range(2):
        for u in range(2):
            loads.append(pltpu.make_async_copy(w_own(f, u), w_at(f, u, z), load_sem.at[2 + 2 * f + u]))
    for load in loads:
        load.start()
    for load in loads:
        load.wait()
    down_pass = remote(down_v.at[0], down_v.at[1], d_send, d_recv, {"blk": 1 - c})
    down_pass.start()

    w_steps(0, 1, 5)
    for i, fwd in ((0, 5), (2, 4)):
        x_copy(i, x_mine(i)).wait_recv()
        x_copy(fwd, x_mine(i)).start()
        x_pass(i).start()
    w_steps(0, 5, last - 1)
    w_step(0, last - 1, "near")
    w_first(1, 1)
    w_step(1, 1, "on")
    w_step(0, last, "end")
    w_step(1, 2, "on")
    for i in (1, 3):
        x_copy(i, x_mine(i)).wait_recv()
        x_pass(i).start()
    compute(0, 0)
    w_step(1, 3, "on")
    for i in range(4):
        x_pass_in(i).wait_recv()
    compute(0, 1)
    w_step(1, 4, "on")
    q_copy(0, 1).start()
    compute(0, 2)
    w_step(1, 5, "on")
    q_copy(0, 2).start()
    w_step(1, 6, "on")
    for i in (4, 5):
        x_copy(i, x_mine(i)).wait_recv()
        x_pass(i).start()
    w_step(1, last - 1, "near")
    for i in (4, 5):
        x_pass_in(i).wait_recv()
    compute(0, 3)
    h_first(0, 0)
    q_copy(0, 3).start()
    for r in (1, 2, 3):
        q_in(0, r).wait_recv()
        h_first(0, r)
    hand_over(0, z)
    w_step(1, last, "end")

    def h_after(f, s):
        for d in range(2):
            hand_over(f, source(s, d))

    h_step(0, 1, "on")
    h_after(0, 1)
    compute(1, 3)
    compute(1, 1)
    q_copy(1, 3).start()
    h_step(0, 2, "on")
    h_after(0, 2)
    q_copy(1, 1).start()
    compute(1, 2)
    compute(1, 0)
    q_copy(1, 2).start()

    def h0_body(s, carry):
        h_step(0, s, "on")
        h_after(0, s)
        return carry
    lax.fori_loop(3, last - 1, h0_body, 0)
    down_pass.wait()
    h_step(0, last - 1, "near")
    h_after(0, last - 1)
    h_first(1, 0)
    for r in (1, 2, 3):
        q_in(1, r).wait_recv()
        h_first(1, r)
    hand_over(1, z)
    h_step(1, 1, "on")
    h_after(1, 1)
    h_step(0, last, "end")
    hand_over(0, source(last, 0))
    finish(z)

    def h1_body(s, carry):
        h_step(1, s, "on")
        h_after(1, s)
        for d in range(2):
            finish(source(s - 1, d))
        return carry
    lax.fori_loop(2, last - 1, h1_body, 0)
    h_step(1, last - 1, "near")
    h_after(1, last - 1)
    for d in range(2):
        finish(source(last - 2, d))
    h_step(1, last, "end")
    hand_over(1, source(last, 0))
    for d in range(2):
        finish(source(last - 1, d))
    finish(source(last, 0))

    for i in range(6):
        x_copy(i, x_mine(i)).wait_send()
        x_pass(i).wait_send()

    def sent(s, carry):
        for f in range(2):
            for d in range(2):
                for u in range(2):
                    w_copy(f, s, u, d, z).wait_send()
                for u in range(4):
                    h_copy(f, s, u, d, z).wait_send()
        return carry
    lax.fori_loop(1, last, sent, 0)
    for f in range(2):
        for d in range(2):
            w_copy(f, last, d, d, z).wait_send()
            for u in range(4):
                if h_takes(u, d):
                    h_copy(f, last, u, d, z).wait_send()
        for r in (1, 2, 3):
            q_copy(f, r).wait_send()

    def leave(i, carry):
        p_copy(0, (1 - c) * last + i).wait_send()
        p_copy(1, (1 - c) * last + i).wait_send()
        out_copy(i).wait()
        return carry
    lax.fori_loop(0, last, leave, 0)


def solution(mesh):
    n = mesh.shape["tp"]
    side = math.isqrt(mesh.shape["groups"])

    def local(tokens, gate, up, down):
        rows, width = tokens.shape
        last = n // 2
        columns = down.shape[1]
        bf16 = jnp.bfloat16
        dma = pltpu.SemaphoreType.DMA
        return pl.pallas_call(
            functools.partial(kernel, side, n),
            out_shape=jax.ShapeDtypeStruct((rows * last, columns), bf16),
            in_specs=[pl.BlockSpec(memory_space=pl.ANY)] * 4,
            out_specs=pl.BlockSpec(memory_space=pl.ANY),
            scratch_shapes=[
                pltpu.VMEM((4, rows, width), bf16),
                pltpu.VMEM((2, width, 2 * UNITS), bf16),
                pltpu.VMEM((n, 2, rows, 4 * UNITS), bf16),
                pltpu.VMEM((last, 2, rows, 4 * UNITS), bf16),
                pltpu.VMEM((2, 3, rows, UNITS), bf16),
                pltpu.VMEM((2, *down.shape), bf16),
                pltpu.VMEM((last, rows, columns), bf16),
                dma((6,)),
                dma((2, 2, last, 2)), dma((2, 2, last, 2)),
                dma((6,)), dma((6,)), dma((6,)), dma((6,)),
                dma((2, 3)), dma((2, 3)),
                dma((2, 2, last, 4)), dma((2, 2, last, 4)),
                dma((last, 2)), dma((last, 2)),
                dma, dma,
                dma((last,)),
            ],
            compiler_params=pltpu.CompilerParams(
                collective_id=0, has_side_effects=True, vmem_limit_bytes=60 * 2**20
            ),
        )(tokens, gate, up, down)

    return jax.shard_map(
        local,
        mesh=mesh,
        in_specs=(P(("groups", "tp"), None), P("tp", "blk"), P("tp", "blk"), P("blk", "tp")),
        out_specs=P(("groups", "blk"), "tp"),
        check_vma=False,
    )
```

```python
import functools
import math

import jax
import jax.numpy as jnp
from jax import lax
from jax.experimental import pallas as pl
from jax.experimental.pallas import tpu as pltpu
from jax.sharding import PartitionSpec as P

MESH = pl.DeviceIdType.MESH
UNITS = 128
SLOTS = 6


def kernel(side, n, tokens, gate, up, down, out, x, w, hid, peer, made, down_v, partial, result,
           load_sem, early, arrived, w_send, x_send, x_recv, xp_send, xp_recv, q_send, q_recv,
           h_send, p_send, p_recv, rest, d_send, d_recv, out_sem):
    last = n // 2
    rows, width = tokens.shape
    depth = gate.shape[0]
    half = gate.shape[1] // 2
    piece = rows // 4

    g = lax.axis_index("groups")
    z = lax.axis_index("tp")
    c = lax.axis_index("blk")
    px = lax.rem(lax.rem(g, side), 2)
    py = lax.rem(lax.div(g, side), 2)
    place = 2 * py + px
    gx = g + 1 - 2 * px
    gy = g + side * (1 - 2 * py)
    gd = gx + side * (1 - 2 * py)
    mates = (None, gx, gy, gd)
    mate_place = (place, 2 * py + 1 - px, 2 * (1 - py) + px, 2 * (1 - py) + 1 - px)
    ahead, behind = lax.rem(z + 1, n), lax.rem(z + n - 1, n)
    to = (ahead, behind)

    def source(s, d):
        return lax.rem(z + n - s, n) if d == 0 else lax.rem(z + s, n)

    barrier = pltpu.get_barrier_semaphore()
    for target in ({"tp": ahead}, {"tp": behind}, {"groups": gx}, {"groups": gy}, {"groups": gd}, {"blk": 1 - c}):
        pl.semaphore_signal(barrier, inc=1, device_id=target, device_id_type=MESH)
    pl.semaphore_wait(barrier, 6)

    def remote(src, dst, send, recv, target):
        return pltpu.make_async_remote_copy(
            src_ref=src, dst_ref=dst, send_sem=send, recv_sem=recv, device_id=target, device_id_type=MESH
        )

    def arrival(half_of, f, s, u, d):
        if f == 0:
            order = last if isinstance(s, int) and s == last else s - 1
        else:
            order = last - 1 if isinstance(s, int) and s == 1 else s + last - 1
        return arrived.at[lax.rem(2 * last * half_of + order, SLOTS), d, u]

    def w_own(f, u):
        first = pl.multiple_of(f * half + place * UNITS, UNITS)
        return (gate, up)[u].at[:, pl.ds(first, UNITS)]

    def w_at(f, u, block):
        return w.at[f, pl.ds(pl.multiple_of(block * depth, 64), depth), pl.ds(u * UNITS, UNITS)]

    def w_copy(f, s, u, d, block, src=None):
        there = w_at(f, u, block)
        first = f == 1 and u == 0 and isinstance(s, int) and s == 1
        return remote(there if src is None else src, there, w_send.at[f],
                      early.at[d] if first else arrival(0, f, s, u, d), {"tp": to[d]})

    def w_first(f, u):
        for d in range(2):
            w_copy(f, 1, u, d, z, w_own(f, u)).start()

    def w_step(f, s, stage):
        for u in range(2):
            for d in range(2):
                if stage == "end" and u != d:
                    continue
                block = source(s, d)
                w_copy(f, s, u, d, block).wait_recv()
                if stage == "on" or (stage == "near" and u == d):
                    w_copy(f, s + 1, u, d, block).start()

    def w_steps(f, low, high):
        def body(s, carry):
            w_step(f, s, "on")
            return carry
        lax.fori_loop(low, high, body, 0)

    def x_rows(core, part):
        return pl.ds(pl.multiple_of(core * (2 * piece) + part * piece, piece), piece)

    pieces = ((1, 0, gx), (1, 1, gx), (2, 1, gy), (2, 0, gy), (3, 1, gx), (3, 0, gy))

    def x_copy(i, src):
        slot, part, target = pieces[i]
        return remote(src, x.at[slot, x_rows(c, part)], x_send, x_recv.at[i], {"groups": target})

    def x_mine(i):
        slot, part, _ = pieces[i]
        return x.at[slot, x_rows(c, part)]

    def x_own(i):
        return tokens.at[x_rows(c, pieces[i][1])]

    def x_pass(i):
        return remote(x_mine(i), x_mine(i), xp_send, xp_recv.at[i], {"blk": 1 - c})

    def x_pass_in(i):
        slot, part, _ = pieces[i]
        there = x.at[slot, x_rows(1 - c, part)]
        return remote(there, there, xp_send, xp_recv.at[i], {"blk": 1 - c})

    def lanes(f, p):
        return pl.ds(pl.multiple_of(f * half + p * UNITS, UNITS), UNITS)

    def compute(f, r):
        both = jnp.dot(x[r], w[f], preferred_element_type=jnp.float32)
        a, b = both[:, :UNITS], both[:, UNITS:]
        h = (a / (1.0 + jnp.exp(-a)) * b).astype(jnp.bfloat16)
        if r == 0:
            hid[z, :, lanes(f, place)] = h
        else:
            made[f, r - 1] = h

    def q_copy(f, r):
        return remote(made.at[f, r - 1], hid.at[z, :, lanes(f, place)],
                      q_send, q_recv.at[f, r - 1], {"groups": mates[r]})

    def q_in(f, r):
        there = hid.at[z, :, lanes(f, mate_place[r])]
        return remote(there, there, q_send, q_recv.at[f, r - 1], {"groups": mates[r]})

    def h_copy(f, s, u, d, block):
        there = hid.at[block, :, lanes(f, mate_place[u])]
        return remote(there, there, h_send.at[f], arrival(1, f, s, u, d), {"tp": to[d]})

    def h_first(f, u):
        for d in range(2):
            h_copy(f, 1, u, d, z).start()

    def h_takes(u, d):
        return u % 2 == d

    def h_step(f, s, stage):
        for u in range(4):
            for d in range(2):
                if stage == "end" and not h_takes(u, d):
                    continue
                block = source(s, d)
                h_copy(f, s, u, d, block).wait_recv()
                if stage == "on" or (stage == "near" and h_takes(u, d)):
                    h_copy(f, s + 1, u, d, block).start()

    def p_copy(first, wide, block, sem=None):
        at = lax.rem(block, last)
        part = pl.ds(first, wide)
        return remote(hid.at[block, :, part], peer.at[at, :, part], p_send,
                      p_recv.at[at] if sem is None else sem, {"blk": 1 - c})

    def is_mine(block):
        return lax.div(block, last) == c

    def hand_over(f, block):
        @pl.when(jnp.logical_not(is_mine(block)))
        def _():
            p_copy(f * half, half, block).start()

    def times(weight, units):
        return lax.dot_general(weight, units, (((1,), (1,)), ((), ())), preferred_element_type=jnp.float32)

    def put_out(block, total):
        columns = pl.ds(pl.multiple_of(lax.rem(block, last) * rows, rows), rows)
        result[:, columns] = total.astype(jnp.bfloat16)
        pltpu.make_async_copy(result.at[:, columns], out.at[:, columns], out_sem).start()

    def finish(block):
        @pl.when(is_mine(block))
        def _():
            p_copy(0, 2 * half, block).wait_recv()
            put_out(block, times(down_v[0], hid[block]) + times(down_v[1], peer[lax.rem(block, last)]))

    def finish_far():
        block = source(last, 0)
        at = lax.rem(block, last)
        parts = [pl.ds(pl.multiple_of(half + row * 2 * UNITS, 2 * UNITS), 2 * UNITS) for row in (py, 1 - py)]

        def both(part):
            return times(down_v[0, :, part], hid[block, :, part]) + times(down_v[1, :, part], peer[at, :, part])

        for i in range(2):
            for d in range(2):
                h_copy(1, last, 2 * i + d, d, block).wait_recv()
            first = pl.multiple_of(half + (py, 1 - py)[i] * 2 * UNITS, 2 * UNITS)
            sem = None if i == 0 else rest

            @pl.when(jnp.logical_not(is_mine(block)))
            def _():
                p_copy(first, 2 * UNITS, block, sem).start()

            @pl.when(is_mine(block))
            def _():
                if i == 0:
                    p_copy(0, half + 2 * UNITS, block).wait_recv()
                    partial[...] = both(pl.ds(0, half)) + both(parts[0])
                else:
                    p_copy(0, 2 * UNITS, block, rest).wait_recv()
                    put_out(block, partial[...] + both(parts[1]))

    w_first(0, 0)
    for i in (0, 2):
        x_copy(i, x_own(i)).start()
    w_first(0, 1)
    for i in (1, 3):
        x_copy(i, x_own(i)).start()
    w_first(1, 0)
    own_rows = pl.ds(pl.multiple_of(z * depth, 64), depth)
    pltpu.make_async_copy(tokens, x.at[0], load_sem.at[0]).start()
    down_load = pltpu.make_async_copy(down, down_v.at[0], load_sem.at[1])
    down_load.start()
    for f in range(2):
        for u in range(2):
            pltpu.make_async_copy(w_own(f, u), w_at(f, u, z), load_sem.at[2]).start()
    w_steps(0, 1, 5)
    pltpu.make_async_copy(tokens, x.at[0], load_sem.at[0]).wait()
    pltpu.make_async_copy(w.at[:, own_rows], w.at[:, own_rows], load_sem.at[2]).wait()
    down_load.wait()
    down_pass = remote(down_v.at[0], down_v.at[1], d_send, d_recv, {"blk": 1 - c})
    down_pass.start()
    for i, fwd in ((0, 5), (2, 4)):
        x_copy(i, x_mine(i)).wait_recv()
        x_copy(fwd, x_mine(i)).start()
        x_pass(i).start()
    w_steps(0, 5, last - 1)
    w_step(0, last - 1, "near")
    w_first(1, 1)
    w_step(1, 1, "on")
    w_step(0, last, "end")
    w_step(1, 2, "on")
    for i in (1, 3):
        x_copy(i, x_mine(i)).wait_recv()
        x_pass(i).start()
    compute(0, 0)
    w_step(1, 3, "on")
    for i in range(4):
        x_pass_in(i).wait_recv()
    compute(0, 1)
    w_step(1, 4, "on")
    q_copy(0, 1).start()
    compute(0, 2)
    w_step(1, 5, "on")
    q_copy(0, 2).start()
    w_step(1, 6, "on")
    for i in (4, 5):
        x_copy(i, x_mine(i)).wait_recv()
        x_pass(i).start()
    w_step(1, last - 1, "near")
    h_first(0, 0)
    for r in (1, 2):
        q_in(0, r).wait_recv()
        h_first(0, r)
    for i in (4, 5):
        x_pass_in(i).wait_recv()
    compute(0, 3)
    q_copy(0, 3).start()
    q_in(0, 3).wait_recv()
    h_first(0, 3)
    hand_over(0, z)
    w_step(1, last, "end")

    def h_after(f, s):
        for d in range(2):
            hand_over(f, source(s, d))

    h_step(0, 1, "on")
    h_after(0, 1)
    compute(1, 3)
    compute(1, 1)
    q_copy(1, 3).start()
    h_step(0, 2, "on")
    h_after(0, 2)
    q_copy(1, 1).start()
    compute(1, 2)
    compute(1, 0)
    q_copy(1, 2).start()

    def h0_body(s, carry):
        h_step(0, s, "on")
        h_after(0, s)
        return carry
    lax.fori_loop(3, last - 1, h0_body, 0)
    down_pass.wait()
    h_step(0, last - 1, "near")
    h_after(0, last - 1)
    h_first(1, 0)
    for r in (1, 2, 3):
        q_in(1, r).wait_recv()
        h_first(1, r)
    hand_over(1, z)
    h_step(1, 1, "on")
    h_after(1, 1)
    h_step(0, last, "end")
    hand_over(0, source(last, 0))
    finish(z)

    def h1_body(s, carry):
        h_step(1, s, "on")
        h_after(1, s)
        for d in range(2):
            finish(source(s - 1, d))
        return carry
    lax.fori_loop(2, last - 1, h1_body, 0)
    h_step(1, last - 1, "near")
    h_after(1, last - 1)
    for d in range(2):
        finish(source(last - 2, d))
    for d in range(2):
        finish(source(last - 1, d))
    finish_far()

    def left(ref, sem):
        remote(ref, ref, sem, rest, {"blk": 1 - c}).wait_send()

    left(x.at[pl.ds(0, 3), pl.ds(0, 2 * piece)], x_send)
    left(x.at[pl.ds(0, 3), pl.ds(0, 2 * piece)], xp_send)
    for f in range(2):
        left(w.at[f, pl.ds(0, (n - 1) * depth)], w_send.at[f])
        left(hid.at[pl.ds(0, n - 1), :, pl.ds(0, half)], h_send.at[f])
    left(made, q_send)
    left(peer, p_send)
    pltpu.make_async_copy(result, out, out_sem).wait()


def solution(mesh):
    n = mesh.shape["tp"]
    side = math.isqrt(mesh.shape["groups"])

    def local(tokens, gate, up, down):
        down = down.T
        rows, width = tokens.shape
        last = n // 2
        columns = down.shape[0]
        bf16 = jnp.bfloat16
        dma = pltpu.SemaphoreType.DMA
        return pl.pallas_call(
            functools.partial(kernel, side, n),
            out_shape=jax.ShapeDtypeStruct((columns, rows * last), bf16),
            in_specs=[pl.BlockSpec(memory_space=pl.ANY)] * 4,
            out_specs=pl.BlockSpec(memory_space=pl.ANY),
            scratch_shapes=[
                pltpu.VMEM((4, rows, width), bf16),
                pltpu.VMEM((2, width, 2 * UNITS), bf16),
                pltpu.VMEM((n, rows, 8 * UNITS), bf16),
                pltpu.VMEM((last, rows, 8 * UNITS), bf16),
                pltpu.VMEM((2, 3, rows, UNITS), bf16),
                pltpu.VMEM((2, *down.shape), bf16),
                pltpu.VMEM((columns, rows), jnp.float32),
                pltpu.VMEM((columns, rows * last), bf16),
                dma((3,)), dma((2,)), dma((SLOTS, 2, 4)), dma((2,)),
                dma, dma((6,)), dma, dma((6,)),
                dma, dma((2, 3)),
                dma((2,)), dma, dma((last,)), dma,
                dma, dma, dma,
            ],
            compiler_params=pltpu.CompilerParams(
                collective_id=0, has_side_effects=True, vmem_limit_bytes=60 * 2**20
            ),
        )(tokens, gate, up, down).T

    return jax.shard_map(
        local,
        mesh=mesh,
        in_specs=(P(("groups", "tp"), None), P("tp", "blk"), P("tp", "blk"), P("blk", "tp")),
        out_specs=P(("groups", "blk"), "tp"),
        check_vma=False,
    )
```

```python
import functools
import math

import jax
import jax.numpy as jnp
from jax import lax
from jax.experimental import pallas as pl
from jax.experimental.pallas import tpu as pltpu
from jax.sharding import PartitionSpec as P

MESH = pl.DeviceIdType.MESH
UNITS = 128
SLOTS = 6


def kernel(side, n, tokens, gate, up, down, out, x, w, hid, peer, made, down_v, partial,
           load_sem, early, arrived, w_send, x_send, x_recv, xp_send, xp_recv, q_send, q_recv,
           h_send, p_send, p_recv, rest, d_send, d_recv):
    last = n // 2
    rows, width = tokens.shape
    depth = gate.shape[0]
    half = gate.shape[1] // 2
    piece = rows // 4

    g = lax.axis_index("groups")
    z = lax.axis_index("tp")
    c = lax.axis_index("blk")
    px = lax.rem(lax.rem(g, side), 2)
    py = lax.rem(lax.div(g, side), 2)
    place = 2 * py + px
    gx = g + 1 - 2 * px
    gy = g + side * (1 - 2 * py)
    gd = gx + side * (1 - 2 * py)
    mates = (None, gx, gy, gd)
    mate_place = (place, 2 * py + 1 - px, 2 * (1 - py) + px, 2 * (1 - py) + 1 - px)
    ahead, behind = lax.rem(z + 1, n), lax.rem(z + n - 1, n)
    to = (ahead, behind)

    def source(s, d):
        return lax.rem(z + n - s, n) if d == 0 else lax.rem(z + s, n)

    barrier = pltpu.get_barrier_semaphore()
    for target in ({"tp": ahead}, {"tp": behind}, {"groups": gx}, {"groups": gy}, {"groups": gd}, {"blk": 1 - c}):
        pl.semaphore_signal(barrier, inc=1, device_id=target, device_id_type=MESH)
    pl.semaphore_wait(barrier, 6)

    def remote(src, dst, send, recv, target):
        return pltpu.make_async_remote_copy(
            src_ref=src, dst_ref=dst, send_sem=send, recv_sem=recv, device_id=target, device_id_type=MESH
        )

    def takes(u, d):
        return u % 2 == d

    def arrival(stage, f, s, u, d):
        if isinstance(s, int) and s == 1:
            return early.at[2 * stage + f, d, u]
        if f == 0:
            order = last if isinstance(s, int) and s == last else s - 1
        else:
            order = s + last - 1
        return arrived.at[lax.rem(2 * last * stage + order, SLOTS), d, u]

    def w_own(f, u):
        first = pl.multiple_of(f * half + place * UNITS, UNITS)
        return (gate, up)[u % 2].at[pl.ds(u // 2 * (depth // 2), depth // 2), pl.ds(first, UNITS)]

    def w_at(f, u, block):
        first = pl.multiple_of(block * depth + u // 2 * (depth // 2), 32)
        return w.at[f, pl.ds(first, depth // 2), pl.ds(u % 2 * UNITS, UNITS)]

    def w_copy(f, s, u, d, block, src=None):
        there = w_at(f, u, block)
        return remote(there if src is None else src, there, w_send.at[f], arrival(0, f, s, u, d), {"tp": to[d]})

    def w_first(f, u):
        for d in range(2):
            w_copy(f, 1, u, d, z, w_own(f, u)).start()

    def w_step(f, s, stage):
        for u in range(4):
            for d in range(2):
                if stage == "end" and not takes(u, d):
                    continue
                block = source(s, d)
                w_copy(f, s, u, d, block).wait_recv()
                if stage == "on" or (stage == "near" and takes(u, d)):
                    w_copy(f, s + 1, u, d, block).start()

    def w_steps(f, low, high):
        def body(s, carry):
            w_step(f, s, "on")
            return carry
        lax.fori_loop(low, high, body, 0)

    def x_rows(core, part):
        return pl.ds(pl.multiple_of(core * (2 * piece) + part * piece, piece), piece)

    pieces = ((1, 0, gx), (1, 1, gx), (2, 1, gy), (2, 0, gy), (3, 1, gx), (3, 0, gy))

    def x_copy(i, src):
        slot, part, target = pieces[i]
        return remote(src, x.at[slot, x_rows(c, part)], x_send, x_recv.at[i], {"groups": target})

    def x_mine(i):
        slot, part, _ = pieces[i]
        return x.at[slot, x_rows(c, part)]

    def x_own(i):
        return tokens.at[x_rows(c, pieces[i][1])]

    def x_pass(i):
        return remote(x_mine(i), x_mine(i), xp_send, xp_recv.at[i], {"blk": 1 - c})

    def x_pass_in(i):
        slot, part, _ = pieces[i]
        there = x.at[slot, x_rows(1 - c, part)]
        return remote(there, there, xp_send, xp_recv.at[i], {"blk": 1 - c})

    def lanes(f, p):
        return pl.ds(pl.multiple_of(f * half + p * UNITS, UNITS), UNITS)

    def compute(f, r):
        both = jnp.dot(x[r], w[f], preferred_element_type=jnp.float32)
        a, b = both[:, :UNITS], both[:, UNITS:]
        h = (a / (1.0 + jnp.exp(-a)) * b).astype(jnp.bfloat16)
        if r == 0:
            hid[z, :, lanes(f, place)] = h
        else:
            made[f, r - 1] = h

    def q_copy(f, r):
        return remote(made.at[f, r - 1], hid.at[z, :, lanes(f, place)],
                      q_send, q_recv.at[f, r - 1], {"groups": mates[r]})

    def q_in(f, r):
        there = hid.at[z, :, lanes(f, mate_place[r])]
        return remote(there, there, q_send, q_recv.at[f, r - 1], {"groups": mates[r]})

    def h_copy(f, s, u, d, block):
        there = hid.at[block, :, lanes(f, mate_place[u])]
        return remote(there, there, h_send.at[f], arrival(1, f, s, u, d), {"tp": to[d]})

    def h_first(f, u):
        for d in range(2):
            h_copy(f, 1, u, d, z).start()

    def h_step(f, s, stage, quarters=range(4)):
        for u in quarters:
            for d in range(2):
                if stage == "end" and not takes(u, d):
                    continue
                block = source(s, d)
                h_copy(f, s, u, d, block).wait_recv()
                if stage == "on" or (stage == "near" and takes(u, d)):
                    h_copy(f, s + 1, u, d, block).start()

    def p_copy(first, wide, block, sem=None):
        at = lax.rem(block, last)
        part = pl.ds(first, wide)
        return remote(hid.at[block, :, part], peer.at[at, :, part], p_send,
                      p_recv.at[at] if sem is None else sem, {"blk": 1 - c})

    def is_mine(block):
        return lax.div(block, last) == c

    def hand_over(f, block):
        @pl.when(jnp.logical_not(is_mine(block)))
        def _():
            p_copy(f * half, half, block).start()

    def times(weight, units):
        return lax.dot_general(weight, units, (((1,), (1,)), ((), ())), preferred_element_type=jnp.float32)

    def put_out(block, total):
        columns = pl.ds(pl.multiple_of(lax.rem(block, last) * rows, rows), rows)
        out[:, columns] = total.astype(jnp.bfloat16)

    def finish(block):
        @pl.when(is_mine(block))
        def _():
            p_copy(0, 2 * half, block).wait_recv()
            put_out(block, times(down_v[0], hid[block]) + times(down_v[1], peer[lax.rem(block, last)]))

    def finish_far():
        block = source(last, 0)
        at = lax.rem(block, last)
        parts = [pl.ds(pl.multiple_of(half + row * 2 * UNITS, 2 * UNITS), 2 * UNITS) for row in (py, 1 - py)]

        def both(part):
            return times(down_v[0, :, part], hid[block, :, part]) + times(down_v[1, :, part], peer[at, :, part])

        for i in range(2):
            for d in range(2):
                h_copy(1, last, 2 * i + d, d, block).wait_recv()
            first = pl.multiple_of(half + (py, 1 - py)[i] * 2 * UNITS, 2 * UNITS)
            sem = None if i == 0 else rest

            @pl.when(jnp.logical_not(is_mine(block)))
            def _():
                p_copy(first, 2 * UNITS, block, sem).start()

            @pl.when(is_mine(block))
            def _():
                if i == 0:
                    p_copy(0, half + 2 * UNITS, block).wait_recv()
                    partial[...] = both(pl.ds(0, half)) + both(parts[0])
                else:
                    p_copy(0, 2 * UNITS, block, rest).wait_recv()
                    put_out(block, partial[...] + both(parts[1]))

    w_first(0, 0)
    w_first(0, 1)
    for i in (0, 2):
        x_copy(i, x_own(i)).start()
    w_first(0, 2)
    w_first(0, 3)
    for i in (1, 3):
        x_copy(i, x_own(i)).start()
    for u in range(4):
        w_first(1, u)
    own_rows = pl.ds(pl.multiple_of(z * depth, 64), depth)
    pltpu.make_async_copy(tokens, x.at[0], load_sem.at[0]).start()
    down_load = pltpu.make_async_copy(down, down_v.at[0], load_sem.at[1])
    down_load.start()
    for f in range(2):
        for u in range(4):
            pltpu.make_async_copy(w_own(f, u), w_at(f, u, z), load_sem.at[2]).start()
    w_step(0, 1, "on")
    w_steps(0, 2, 5)
    pltpu.make_async_copy(tokens, x.at[0], load_sem.at[0]).wait()
    pltpu.make_async_copy(w.at[:, own_rows], w.at[:, own_rows], load_sem.at[2]).wait()
    down_load.wait()
    down_pass = remote(down_v.at[0], down_v.at[1], d_send, d_recv, {"blk": 1 - c})
    down_pass.start()
    for i, fwd in ((0, 5), (2, 4)):
        x_copy(i, x_mine(i)).wait_recv()
        x_copy(fwd, x_mine(i)).start()
        x_pass(i).start()
    w_steps(0, 5, last - 1)
    w_step(0, last - 1, "near")
    w_step(1, 1, "on")
    w_step(0, last, "end")
    compute(0, 0)
    for i in (1, 3):
        x_copy(i, x_mine(i)).wait_recv()
        x_pass(i).start()
    h_first(0, 0)
    w_step(1, 2, "on")
    for i in range(4):
        x_pass_in(i).wait_recv()
    compute(0, 1)
    w_step(1, 3, "on")
    q_copy(0, 1).start()
    compute(0, 2)
    w_step(1, 4, "on")
    q_copy(0, 2).start()
    q_in(0, 1).wait_recv()
    h_first(0, 1)
    w_step(1, 5, "on")
    for i in (4, 5):
        x_copy(i, x_mine(i)).wait_recv()
        x_pass(i).start()
    q_in(0, 2).wait_recv()
    h_first(0, 2)
    w_step(1, 6, "on")
    for i in (4, 5):
        x_pass_in(i).wait_recv()
    compute(0, 3)
    q_copy(0, 3).start()
    h_step(0, 1, "on", (0, 1))
    w_step(1, last - 1, "near")
    h_step(0, 1, "on", (2,))
    q_in(0, 3).wait_recv()
    h_first(0, 3)
    hand_over(0, z)
    w_step(1, last, "end")

    def h_after(f, s):
        for d in range(2):
            hand_over(f, source(s, d))

    for s in range(1, 7):
        h_step(0, s, "on", (3,) if s == 1 else range(4))
        h_after(0, s)
        if 2 < s < 6:
            q_copy(1, (3, 1, 2)[s - 3]).start()
        if 1 < s < 6:
            compute(1, (3, 1, 2, 0)[s - 2])
    h_first(1, 0)
    for r in (1, 2, 3):
        q_in(1, r).wait_recv()
        h_first(1, r)
    hand_over(1, z)
    h_step(0, last - 1, "near")
    h_after(0, last - 1)
    down_pass.wait()
    h_step(1, 1, "on")
    h_after(1, 1)
    h_step(0, last, "end")
    hand_over(0, source(last, 0))
    finish(z)
    h_step(1, 2, "on")
    h_after(1, 2)

    def h1_step(s, stage):
        h_step(1, s, stage, (0, 1))
        for d in range(2):
            finish(source(s - 2, d))
        h_step(1, s, stage, (2, 3))
        h_after(1, s)

    def h1_body(s, carry):
        h1_step(s, "on")
        return carry
    lax.fori_loop(3, last - 1, h1_body, 0)
    h1_step(last - 1, "near")
    for s in (last - 2, last - 1):
        for d in range(2):
            finish(source(s, d))
    finish_far()

    def left(ref, sem):
        remote(ref, ref, sem, rest, {"blk": 1 - c}).wait_send()

    left(x.at[pl.ds(0, 3), pl.ds(0, 2 * piece)], x_send)
    left(x.at[pl.ds(0, 3), pl.ds(0, 2 * piece)], xp_send)
    for f in range(2):
        left(w.at[f, pl.ds(0, (n - 1) * depth)], w_send.at[f])
        left(hid.at[pl.ds(0, n - 1), :, pl.ds(0, half)], h_send.at[f])
    left(made, q_send)
    left(peer, p_send)


def solution(mesh):
    n = mesh.shape["tp"]
    side = math.isqrt(mesh.shape["groups"])

    def local(tokens, gate, up, down):
        down = down.T
        rows, width = tokens.shape
        last = n // 2
        columns = down.shape[0]
        bf16 = jnp.bfloat16
        dma = pltpu.SemaphoreType.DMA
        return pl.pallas_call(
            functools.partial(kernel, side, n),
            out_shape=jax.ShapeDtypeStruct((columns, rows * last), bf16),
            in_specs=[pl.BlockSpec(memory_space=pltpu.HBM)] * 4,
            out_specs=pl.BlockSpec(memory_space=pltpu.VMEM),
            scratch_shapes=[
                pltpu.VMEM((4, rows, width), bf16),
                pltpu.VMEM((2, width, 2 * UNITS), bf16),
                pltpu.VMEM((n, rows, 8 * UNITS), bf16),
                pltpu.VMEM((last, rows, 8 * UNITS), bf16),
                pltpu.VMEM((2, 3, rows, UNITS), bf16),
                pltpu.VMEM((2, *down.shape), bf16),
                pltpu.VMEM((columns, rows), jnp.float32),
                dma((3,)), dma((4, 2, 4)), dma((SLOTS, 2, 4)), dma((2,)),
                dma, dma((6,)), dma, dma((6,)),
                dma, dma((2, 3)),
                dma((2,)), dma, dma((last,)), dma,
                dma, dma,
            ],
            compiler_params=pltpu.CompilerParams(
                collective_id=0, has_side_effects=True, vmem_limit_bytes=44 * 2**20
            ),
        )(*[pltpu.with_memory_space_constraint(a, pltpu.HBM) for a in (tokens, gate, up, down)]).T

    return jax.shard_map(
        local,
        mesh=mesh,
        in_specs=(P(("groups", "tp"), None), P("tp", "blk"), P("tp", "blk"), P("blk", "tp")),
        out_specs=P(("groups", "blk"), "tp"),
        check_vma=False,
    )
```

```python
import functools
import math

import jax
import jax.numpy as jnp
from jax import lax
from jax.experimental import pallas as pl
from jax.experimental.pallas import tpu as pltpu
from jax.sharding import PartitionSpec as P

MESH = pl.DeviceIdType.MESH
UNITS = 128
SLOTS = 6


def kernel(side, n, tokens, gate, up, down, out, x, w, hid, peer, made, down_v, partial,
           load_sem, early, arrived, w_send, x_send, x_recv, xp_send, xp_recv, q_send, q_recv,
           h_send, p_send, p_recv, rest, d_send, d_recv):
    last = n // 2
    rows, width = tokens.shape
    depth = gate.shape[0]
    half = gate.shape[1] // 2
    piece = rows // 4

    g = lax.axis_index("groups")
    z = lax.axis_index("tp")
    c = lax.axis_index("blk")
    px = lax.rem(lax.rem(g, side), 2)
    py = lax.rem(lax.div(g, side), 2)
    place = 2 * py + px
    gx = g + 1 - 2 * px
    gy = g + side * (1 - 2 * py)
    gd = gx + side * (1 - 2 * py)
    mates = (None, gx, gy, gd)
    mate_place = (place, 2 * py + 1 - px, 2 * (1 - py) + px, 2 * (1 - py) + 1 - px)
    ahead, behind = lax.rem(z + 1, n), lax.rem(z + n - 1, n)
    to = (ahead, behind)

    def source(s, d):
        return lax.rem(z + n - s, n) if d == 0 else lax.rem(z + s, n)

    def remote(src, dst, send, recv, target):
        return pltpu.make_async_remote_copy(
            src_ref=src, dst_ref=dst, send_sem=send, recv_sem=recv, device_id=target, device_id_type=MESH
        )

    def takes(u, d):
        return u % 2 == d

    def arrival(stage, f, s, u, d):
        if isinstance(s, int) and s == 1:
            return early.at[2 * stage + f, d, u]
        if f == 0:
            order = last if isinstance(s, int) and s == last else s - 1
        else:
            order = s + last - 1
        return arrived.at[lax.rem(2 * last * stage + order, SLOTS), d, u]

    def w_own(f, u):
        first = pl.multiple_of(f * half + place * UNITS, UNITS)
        return (gate, up)[u % 2].at[pl.ds(u // 2 * (depth // 2), depth // 2), pl.ds(first, UNITS)]

    def w_at(f, u, block):
        first = pl.multiple_of(block * depth + u // 2 * (depth // 2), 32)
        return w.at[f, pl.ds(first, depth // 2), pl.ds(u % 2 * UNITS, UNITS)]

    def w_copy(f, s, u, d, block):
        there = w_at(f, u, block)
        return remote(there, there, w_send.at[f], arrival(0, f, s, u, d), {"tp": to[d]})

    def w_first(f, u):
        for d in range(2):
            w_copy(f, 1, u, d, z).start()

    def w_step(f, s, stage):
        for u in range(4):
            for d in range(2):
                if stage == "end" and not takes(u, d):
                    continue
                block = source(s, d)
                w_copy(f, s, u, d, block).wait_recv()
                if stage == "on" or (stage == "near" and takes(u, d)):
                    w_copy(f, s + 1, u, d, block).start()

    def w_steps(f, low, high):
        def body(s, carry):
            w_step(f, s, "on")
            return carry
        lax.fori_loop(low, high, body, 0)

    def x_rows(core, part):
        return pl.ds(pl.multiple_of(core * (2 * piece) + part * piece, piece), piece)

    pieces = ((1, 0, gx), (1, 1, gx), (2, 1, gy), (2, 0, gy), (3, 1, gx), (3, 0, gy))

    def x_copy(i, src):
        slot, part, target = pieces[i]
        return remote(src, x.at[slot, x_rows(c, part)], x_send, x_recv.at[i], {"groups": target})

    def x_mine(i):
        slot, part, _ = pieces[i]
        return x.at[slot, x_rows(c, part)]

    def x_own(i):
        return x.at[0, x_rows(c, pieces[i][1])]

    def x_pass(i):
        return remote(x_mine(i), x_mine(i), xp_send, xp_recv.at[i], {"blk": 1 - c})

    def x_pass_in(i):
        slot, part, _ = pieces[i]
        there = x.at[slot, x_rows(1 - c, part)]
        return remote(there, there, xp_send, xp_recv.at[i], {"blk": 1 - c})

    def lanes(f, p):
        return pl.ds(pl.multiple_of(f * half + p * UNITS, UNITS), UNITS)

    def compute(f, r):
        both = jnp.dot(x[r], w[f], preferred_element_type=jnp.float32)
        a, b = both[:, :UNITS], both[:, UNITS:]
        h = (a / (1.0 + jnp.exp(-a)) * b).astype(jnp.bfloat16)
        if r == 0:
            hid[z, :, lanes(f, place)] = h
        else:
            made[f, r - 1] = h

    def q_copy(f, r):
        return remote(made.at[f, r - 1], hid.at[z, :, lanes(f, place)],
                      q_send, q_recv.at[f, r - 1], {"groups": mates[r]})

    def q_in(f, r):
        there = hid.at[z, :, lanes(f, mate_place[r])]
        return remote(there, there, q_send, q_recv.at[f, r - 1], {"groups": mates[r]})

    def h_copy(f, s, u, d, block):
        there = hid.at[block, :, lanes(f, mate_place[u])]
        return remote(there, there, h_send.at[f], arrival(1, f, s, u, d), {"tp": to[d]})

    def h_first(f, u):
        for d in range(2):
            h_copy(f, 1, u, d, z).start()

    def h_step(f, s, stage, quarters=range(4)):
        for u in quarters:
            for d in range(2):
                if stage == "end" and not takes(u, d):
                    continue
                block = source(s, d)
                h_copy(f, s, u, d, block).wait_recv()
                if stage == "on" or (stage == "near" and takes(u, d)):
                    h_copy(f, s + 1, u, d, block).start()

    def p_copy(first, wide, block, sem=None):
        at = lax.rem(block, last)
        part = pl.ds(first, wide)
        return remote(hid.at[block, :, part], peer.at[at, :, part], p_send,
                      p_recv.at[at] if sem is None else sem, {"blk": 1 - c})

    def is_mine(block):
        return lax.div(block, last) == c

    def hand_over(f, block):
        @pl.when(jnp.logical_not(is_mine(block)))
        def _():
            p_copy(f * half, half, block).start()

    def times(weight, units):
        return lax.dot_general(weight, units, (((1,), (1,)), ((), ())), preferred_element_type=jnp.float32)

    def put_out(block, total):
        columns = pl.ds(pl.multiple_of(lax.rem(block, last) * rows, rows), rows)
        out[:, columns] = total.astype(jnp.bfloat16)

    def finish(block):
        @pl.when(is_mine(block))
        def _():
            p_copy(0, 2 * half, block).wait_recv()
            put_out(block, times(down_v[0], hid[block]) + times(down_v[1], peer[lax.rem(block, last)]))

    def finish_far():
        block = source(last, 0)
        at = lax.rem(block, last)
        parts = [pl.ds(pl.multiple_of(half + row * 2 * UNITS, 2 * UNITS), 2 * UNITS) for row in (py, 1 - py)]

        def both(part):
            return times(down_v[0, :, part], hid[block, :, part]) + times(down_v[1, :, part], peer[at, :, part])

        for i in range(2):
            for d in range(2):
                h_copy(1, last, 2 * i + d, d, block).wait_recv()
            first = pl.multiple_of(half + (py, 1 - py)[i] * 2 * UNITS, 2 * UNITS)
            sem = None if i == 0 else rest

            @pl.when(jnp.logical_not(is_mine(block)))
            def _():
                p_copy(first, 2 * UNITS, block, sem).start()

            @pl.when(is_mine(block))
            def _():
                if i == 0:
                    p_copy(0, half + 2 * UNITS, block).wait_recv()
                    partial[...] = both(pl.ds(0, half)) + both(parts[0])
                else:
                    p_copy(0, 2 * UNITS, block, rest).wait_recv()
                    put_out(block, partial[...] + both(parts[1]))

    own_rows = pl.ds(pl.multiple_of(z * depth, 64), depth)
    for f in range(2):
        for u in range(4):
            pltpu.make_async_copy(w_own(f, u), w_at(f, u, z), load_sem.at[f]).start()
    tokens_load = pltpu.make_async_copy(tokens, x.at[0], load_sem.at[2])
    tokens_load.start()
    down_load = pltpu.make_async_copy(down, down_v.at[0], load_sem.at[3])
    down_load.start()

    barrier = pltpu.get_barrier_semaphore()
    for target in ({"tp": ahead}, {"tp": behind}, {"groups": gx}, {"groups": gy}, {"groups": gd}, {"blk": 1 - c}):
        pl.semaphore_signal(barrier, inc=1, device_id=target, device_id_type=MESH)
    pl.semaphore_wait(barrier, 6)

    for f in range(2):
        there = w.at[f, own_rows]
        pltpu.make_async_copy(there, there, load_sem.at[f]).wait()
        if f == 0:
            w_first(0, 0)
            w_first(0, 1)
    tokens_load.wait()
    for i in (0, 2):
        x_copy(i, x_own(i)).start()
    w_first(0, 2)
    w_first(0, 3)
    for i in (1, 3):
        x_copy(i, x_own(i)).start()
    for u in range(4):
        w_first(1, u)
    w_step(0, 1, "on")
    w_steps(0, 2, 5)
    down_load.wait()
    down_pass = remote(down_v.at[0], down_v.at[1], d_send, d_recv, {"blk": 1 - c})
    down_pass.start()
    for i, fwd in ((0, 5), (2, 4)):
        x_copy(i, x_mine(i)).wait_recv()
        x_copy(fwd, x_mine(i)).start()
        x_pass(i).start()
    w_steps(0, 5, last - 1)
    w_step(0, last - 1, "near")
    w_step(1, 1, "on")
    w_step(0, last, "end")
    compute(0, 0)
    for i in (1, 3):
        x_copy(i, x_mine(i)).wait_recv()
        x_pass(i).start()
    h_first(0, 0)
    w_step(1, 2, "on")
    for i in range(4):
        x_pass_in(i).wait_recv()
    compute(0, 1)
    w_step(1, 3, "on")
    q_copy(0, 1).start()
    compute(0, 2)
    w_step(1, 4, "on")
    q_copy(0, 2).start()
    q_in(0, 1).wait_recv()
    h_first(0, 1)
    w_step(1, 5, "on")
    for i in (4, 5):
        x_copy(i, x_mine(i)).wait_recv()
        x_pass(i).start()
    q_in(0, 2).wait_recv()
    h_first(0, 2)
    w_step(1, 6, "on")
    for i in (4, 5):
        x_pass_in(i).wait_recv()
    compute(0, 3)
    q_copy(0, 3).start()
    h_step(0, 1, "on", (0, 1))
    w_step(1, last - 1, "near")
    h_step(0, 1, "on", (2,))
    q_in(0, 3).wait_recv()
    h_first(0, 3)
    hand_over(0, z)
    h_step(0, 2, "on", (0, 1))
    w_step(1, last, "end")
    h_step(0, 2, "on", (2,))

    def h_after(f, s):
        for d in range(2):
            hand_over(f, source(s, d))

    h_step(0, 1, "on", (3,))
    h_after(0, 1)
    for s in range(3, last):
        h_step(0, s, "on" if s < last - 1 else "near", range(3))
        h_step(0, s - 1, "on", (3,))
        h_after(0, s - 1)
        if 3 < s < 7:
            q_copy(1, (3, 1, 2)[s - 4]).start()
        if s < 7:
            compute(1, (3, 1, 2, 0)[s - 3])
    h_first(1, 0)
    for r in (1, 2, 3):
        q_in(1, r).wait_recv()
        h_first(1, r)
    hand_over(1, z)
    h_step(0, last - 1, "near", (3,))
    h_after(0, last - 1)
    down_pass.wait()
    h_step(1, 1, "on")
    h_after(1, 1)
    h_step(0, last, "end")
    hand_over(0, source(last, 0))
    finish(z)
    h_step(1, 2, "on")
    h_after(1, 2)

    def h1_step(s, stage):
        h_step(1, s, stage, (0, 1))
        for d in range(2):
            finish(source(s - 2, d))
        h_step(1, s, stage, (2, 3))
        h_after(1, s)

    def h1_body(s, carry):
        h1_step(s, "on")
        return carry
    lax.fori_loop(3, last - 1, h1_body, 0)
    h1_step(last - 1, "near")
    for s in (last - 2, last - 1):
        for d in range(2):
            finish(source(s, d))
    finish_far()

    def left(ref, sem):
        remote(ref, ref, sem, rest, {"blk": 1 - c}).wait_send()

    left(x.at[pl.ds(0, 3), pl.ds(0, 2 * piece)], x_send)
    left(x.at[pl.ds(0, 3), pl.ds(0, 2 * piece)], xp_send)
    for f in range(2):
        left(w.at[f, pl.ds(0, (n - 1) * depth)], w_send.at[f])
        left(hid.at[pl.ds(0, n - 1), :, pl.ds(0, half)], h_send.at[f])
    left(made, q_send)
    left(peer, p_send)


def solution(mesh):
    n = mesh.shape["tp"]
    side = math.isqrt(mesh.shape["groups"])

    def local(tokens, gate, up, down):
        down = down.T
        rows, width = tokens.shape
        last = n // 2
        columns = down.shape[0]
        bf16 = jnp.bfloat16
        dma = pltpu.SemaphoreType.DMA
        return pl.pallas_call(
            functools.partial(kernel, side, n),
            out_shape=jax.ShapeDtypeStruct((columns, rows * last), bf16),
            in_specs=[pl.BlockSpec(memory_space=pltpu.HBM)] * 4,
            out_specs=pl.BlockSpec(memory_space=pltpu.VMEM),
            scratch_shapes=[
                pltpu.VMEM((4, rows, width), bf16),
                pltpu.VMEM((2, width, 2 * UNITS), bf16),
                pltpu.VMEM((n, rows, 8 * UNITS), bf16),
                pltpu.VMEM((last, rows, 8 * UNITS), bf16),
                pltpu.VMEM((2, 3, rows, UNITS), bf16),
                pltpu.VMEM((2, *down.shape), bf16),
                pltpu.VMEM((columns, rows), jnp.float32),
                dma((4,)), dma((4, 2, 4)), dma((SLOTS, 2, 4)), dma((2,)),
                dma, dma((6,)), dma, dma((6,)),
                dma, dma((2, 3)),
                dma((2,)), dma, dma((last,)), dma,
                dma, dma,
            ],
            compiler_params=pltpu.CompilerParams(
                collective_id=0, has_side_effects=True, vmem_limit_bytes=44 * 2**20
            ),
        )(*[pltpu.with_memory_space_constraint(a, pltpu.HBM) for a in (tokens, gate, up, down)]).T

    return jax.shard_map(
        local,
        mesh=mesh,
        in_specs=(P(("groups", "tp"), None), P("tp", "blk"), P("tp", "blk"), P("blk", "tp")),
        out_specs=P(("groups", "blk"), "tp"),
        check_vma=False,
    )
```
